32 devices in a mesh: prompt: 8 (over z, core), ctx: 4 (over y, x).
Axes of the slice: x: 2, y: 2, z: 4, core: 2. Of those that a mesh axis runs over, the one named last changes fastest.
Arguments:
- queries: bfloat16 [16384, 16, 128], P(('prompt', 'ctx')), may hold values from -8 to 8
- keys: bfloat16 [16384, 4, 128], P(('prompt', 'ctx')), may hold values from -8 to 8
- values: bfloat16 [16384, 4, 128], P(('prompt', 'ctx')), may hold values from -6 to 6
- spans: int32 [8, 2], P('prompt'), may hold values from 1 to 1536, as said below
- partner: int32 [8], replicated, may hold values from 0 to 7, each once
Outputs:
- attended: bfloat16 [16384, 16, 128], P(('prompt', 'ctx'))
- decode_cache: bfloat16 [8, 2, 8, 4, 256, 128], P('ctx', None, 'prompt')
The draws below stay inside these ranges and needn't reach their ends.
Inputs may be any that keep to these rules, and one draw needn't show every extreme that they name: `spans`: column 0 counts the image tokens of a prompt, from 512 to 1024, which come first; column 1 counts the text tokens after them, 1 or more; the two sum to at most 2048, and to exactly 2048 for at least one prompt.
All inputs are finite; a program needn't handle non-finite values.
Results may differ from the reference program's by a relative error of at most 0.0041.
Values may be sent and summed in bfloat16 or wider, within the bound.
A program may use at most 64 MiB of HBM per device.

```python
import math
import jax
import jax.numpy as jnp
from jax import lax

HEADS = 16
KVH = 4
HD = 128
SEQ = 2048
PROMPTS = 8
TOKENS = 16384
STRIPES = 2
BLOCKS = 4
ROWS_STRIPE = 256


def draw_queries(key, part):
    drawn = jnp.clip(jax.random.normal(jax.random.fold_in(key, 11), (TOKENS, HEADS, HD), jnp.float32), -4.0, 4.0)
    return drawn.astype(jnp.bfloat16)


def draw_keys(key, part):
    drawn = jnp.clip(jax.random.normal(jax.random.fold_in(key, 21), (TOKENS, KVH, HD), jnp.float32), -4.0, 4.0)
    return drawn.astype(jnp.bfloat16)


def draw_spans(key, part):
    image_count = jax.random.randint(jax.random.fold_in(key, 31), (PROMPTS,), SEQ // 4, SEQ // 2 + 1)
    text_count = jax.random.randint(jax.random.fold_in(key, 32), (PROMPTS,), 1, SEQ - image_count + 1)
    fullest = jax.random.randint(jax.random.fold_in(key, 33), (), 0, PROMPTS)
    shortest = (fullest + 1) % PROMPTS
    index_row = jnp.arange(PROMPTS)
    image_count = jnp.where(index_row == fullest, SEQ // 4, image_count)
    text_count = jnp.where(index_row == fullest, SEQ - SEQ // 4, text_count)
    text_count = jnp.where(index_row == shortest, 1, text_count)
    return jnp.stack([image_count, text_count], axis=1).astype(jnp.int32)


def levels(key, dims, split, smallest, top_value):
    def one(position, parts):
        draws = jax.random.uniform(jax.random.fold_in(jax.random.fold_in(key, 6), position), (parts,), jnp.float32, smallest / len(split), top_value / len(split))
        return jnp.repeat(jnp.exp(draws), dims[position] // parts).reshape((-1,) + (1,) * (len(dims) - position - 1))

    gain = one(*split[0])
    for cut in split[1:]:
        gain = gain * one(*cut)
    return gain


def scatter_about(stream_key, dims, scale, most, cuts=(), kind=jnp.bfloat16):
    values = scale * jax.random.normal(stream_key, dims, jnp.float32)
    if cuts:
        values = values * levels(stream_key, dims, cuts, -0.22, 0.18)
    return jnp.clip(values, -most, most).astype(kind)


def setup_inputs(seed: int = 0) -> dict:
    key_list = jax.random.split(jax.random.key(seed), 6)
    return {
        "queries": draw_queries(jax.random.fold_in(key_list[5], 71), 0),
        "keys": draw_keys(jax.random.fold_in(key_list[5], 71), 0),
        "values": scatter_about(key_list[2], (TOKENS, KVH, HD), 1.0, 6.0, ((0, 32),)),
        "spans": draw_spans(jax.random.fold_in(key_list[5], 71), 0),
        "partner": jax.random.permutation(key_list[4], PROMPTS).astype(jnp.int32),
    }


def attend_prompt(prompt_item):
    prompt_queries, prompt_keys, prompt_values, length = prompt_item
    qblock = math.gcd(SEQ, 512)
    block_count = SEQ // qblock
    members = HEADS // KVH
    grouped = prompt_queries.reshape(block_count, qblock, KVH, members, HD)
    keys_wide = prompt_keys.astype(jnp.float32)
    values_wide = prompt_values.astype(jnp.float32)
    key_pos = lax.iota(jnp.int32, SEQ)

    def one_block(block_item):
        query_block, block_index = block_item
        query_pos = block_index * qblock + lax.iota(jnp.int32, qblock)
        scores = jnp.einsum('qgmd,kgd->qgmk', query_block.astype(jnp.float32), keys_wide) * (1.0 / math.sqrt(HD))
        allowed = ((key_pos[None, :] <= query_pos[:, None]) & (key_pos[None, :] < length))[:, None, None, :]
        scores = jnp.where(allowed, scores, -1e+30)
        row_peak = lax.optimization_barrier(jnp.max(scores, axis=-1, keepdims=True))
        weights = jnp.where(allowed, jnp.exp(scores - row_peak), 0.0)
        rounded = lax.optimization_barrier(weights.astype(jnp.bfloat16)).astype(jnp.float32)
        mixture = jnp.einsum('qgmk,kgd->qgmd', rounded, values_wide) / lax.optimization_barrier(jnp.sum(weights, axis=-1))[..., None]
        mixture = jnp.where((query_pos < length)[:, None, None, None], mixture, 0.0)
        return mixture.reshape(qblock, HEADS, HD).astype(jnp.bfloat16)
    finished = lax.map(one_block, (grouped, jnp.arange(block_count, dtype=jnp.int32)))
    return finished.reshape(SEQ, HEADS, HD)

def reference(queries, keys, values, spans, partner):
    lengths = spans[:, 0] + spans[:, 1]
    prompt_queries = queries.reshape(PROMPTS, SEQ, HEADS, HD)
    prompt_keys = keys.reshape(PROMPTS, SEQ, KVH, HD)
    prompt_values = values.reshape(PROMPTS, SEQ, KVH, HD)
    attended = lax.map(attend_prompt, (prompt_queries, prompt_keys, prompt_values, lengths))
    attended = attended.reshape(TOKENS, HEADS, HD)
    live_rows = (lax.iota(jnp.int32, SEQ)[None, :] < lengths[:, None])[:, :, None, None]
    paired = jnp.stack([jnp.where(live_rows, prompt_keys, jnp.zeros_like(prompt_keys)), jnp.where(live_rows, prompt_values, jnp.zeros_like(prompt_values))], axis=1)
    paired = jnp.take(paired, partner.astype(jnp.int32), axis=0)
    paired = paired.reshape(PROMPTS, 2, BLOCKS, ROWS_STRIPE, STRIPES, KVH, HD)
    decode_cache = paired.transpose(0, 1, 4, 5, 2, 3, 6).reshape(PROMPTS, 2, STRIPES * KVH, BLOCKS, ROWS_STRIPE, HD)
    return (attended, decode_cache)
```

```python
import functools
import math

import jax
import jax.numpy as jnp
from jax import lax
from jax.experimental import pallas as pl
from jax.experimental.pallas import tpu as pltpu
from jax.sharding import PartitionSpec as P

far_below = -1e30
MESH = pl.DeviceIdType.MESH
f32, bf16 = jnp.float32, jnp.bfloat16


def prep_kernel(spans_ref, base_ref, k_ref, v_ref, out_ref, tmp):
    groups, _, stripes, rows, _ = out_ref.shape
    length = spans_ref[0, 0] + spans_ref[0, 1]
    row = lax.broadcasted_iota(jnp.int32, (rows, 1), 0)
    for t, ref in enumerate((k_ref, v_ref)):
        tmp[t] = ref[...].astype(f32)
        for st in range(stripes):
            live = base_ref[0] + row * stripes + st < length
            for g in range(groups):
                x = tmp[t, pl.ds(st * groups + g, rows, stride=stripes * groups), :]
                out_ref[g, t, st] = jnp.where(live, x, 0.0).astype(bf16)


def main_kernel(
    n_prompt,
    n_ctx,
    spans_ref,
    partner_ref,
    q_ref,
    kv_ref,
    att_ref,
    dec_ref,
    kvbuf,
    hand1,
    hand2,
    tmp,
    qh,
    acc,
    peak,
    bias,
    own_sem,
    kv_send,
    kv_recv,
    h1_send,
    h1_recv,
    h2_send,
    h2_recv,
):
    tok, heads, width = q_ref.shape
    groups, _, stripes, rows, _ = kv_ref.shape
    members = heads // groups
    per_ctx = dec_ref.shape[0]
    me_p = lax.axis_index("prompt")
    me = lax.axis_index("ctx")
    length = spans_ref[0, 0] + spans_ref[0, 1]
    scale = math.log2(math.e) / math.sqrt(width)

    own = pltpu.make_async_copy(kv_ref, kvbuf.at[me], own_sem)
    own.start()

    barrier = pltpu.get_barrier_semaphore()
    for k in range(1, n_prompt):
        pl.semaphore_signal(
            barrier, inc=1, device_id={"prompt": lax.rem(me_p + k, n_prompt)}, device_id_type=MESH
        )
    for k in range(1, n_ctx):
        pl.semaphore_signal(
            barrier, inc=1, device_id={"ctx": lax.rem(me + k, n_ctx)}, device_id_type=MESH
        )
    own.wait()
    pl.semaphore_wait(barrier, n_prompt + n_ctx - 2)

    def kv_copy(dest, block, g):
        return pltpu.make_async_remote_copy(
            src_ref=kvbuf.at[block, g],
            dst_ref=kvbuf.at[block, g],
            send_sem=kv_send.at[dest, g],
            recv_sem=kv_recv.at[block, g],
            device_id={"ctx": dest},
            device_id_type=MESH,
        )

    def h1_copy(slot):
        return pltpu.make_async_remote_copy(
            src_ref=kvbuf.at[me, lax.rem(slot, groups), :, lax.div(slot, groups)],
            dst_ref=hand1.at[me_p],
            send_sem=h1_send.at[slot],
            recv_sem=h1_recv.at[me_p],
            device_id={"prompt": slot},
            device_id_type=MESH,
        )

    def h2_copy(dest):
        return pltpu.make_async_remote_copy(
            src_ref=hand2.at[pl.ds(dest * per_ctx, per_ctx)],
            dst_ref=dec_ref.at[:, :, 0, me],
            send_sem=h2_send.at[dest],
            recv_sem=h2_recv.at[me],
            device_id={"ctx": dest},
            device_id_type=MESH,
        )

    own1 = pltpu.make_async_copy(
        kvbuf.at[me, lax.rem(me_p, groups), :, lax.div(me_p, groups)],
        hand1.at[me_p],
        h1_send.at[me_p],
    )
    own2 = pltpu.make_async_copy(
        hand2.at[pl.ds(me * per_ctx, per_ctx)], dec_ref.at[:, :, 0, me], h2_send.at[me]
    )

    def send_group(g, carry):
        def send_one(k, carry):
            kv_copy(n_ctx - k, me, g).start()
            return carry

        lax.fori_loop(1, n_ctx - me, send_one, 0)
        return carry

    lax.fori_loop(0, groups, send_group, 0)
    own1.start()
    for k in range(1, n_prompt):
        h1_copy(lax.rem(me_p + k, n_prompt)).start()

    tmp[...] = q_ref[...].reshape(tok * heads, width).astype(f32)
    for h in range(heads):
        qh[h] = tmp[pl.ds(h, tok, stride=heads), :].astype(bf16)
    col = lax.broadcasted_iota(jnp.int32, (1, tok), 1)
    key_pos = lax.rem(col, rows) * stripes + lax.div(col, rows)
    row_pos = lax.broadcasted_iota(jnp.int32, (tok, 1), 0)
    bias[...] = jnp.where(
        (key_pos <= row_pos) & (key_pos + me * tok < length), 0.0, far_below
    )
    ones = jnp.ones((tok, width), bf16)
    tile = tok // 2

    def attend(block, g, first):
        keys = kvbuf[block, g, 0].reshape(tok, width)
        mixed = jnp.concatenate([kvbuf[block, g, 1].reshape(tok, width), ones], axis=1)
        if not first:
            row_bias = jnp.where(key_pos + block * tok < length, 0.0, far_below)

        def one_head(m, carry):
            h = g * members + m
            for start in range(0, tok, tile):
                part = pl.ds(start, tile)
                scores = lax.dot_general(
                    qh[h, part, :], keys, (((1,), (1,)), ((), ())), preferred_element_type=f32
                )
                scores = scores * scale + (bias[part, :] if first else row_bias)
                top = jnp.max(scores, axis=1, keepdims=True)
                if not first:
                    before = peak[h, part, :]
                    top = jnp.maximum(top, before)
                weights = jnp.exp2(scores - top).astype(bf16)
                mixture = jnp.dot(weights, mixed, preferred_element_type=f32)
                if not first:
                    mixture = mixture + acc[h, part, :] * jnp.exp2(before - top)
                acc[h, part, :] = mixture
                peak[h, part, :] = top
            return carry

        lax.fori_loop(0, members, one_head, 0)

    def diagonal(g, carry):
        attend(me, g, True)
        return carry

    lax.fori_loop(0, groups, diagonal, 0)

    def stage_two():
        own1.wait()
        for k in range(1, n_prompt):
            h1_copy(lax.rem(me_p + k, n_prompt)).wait_send()
        for k in range(1, n_prompt):
            source = lax.rem(me_p + k, n_prompt)
            pltpu.make_async_copy(hand1.at[source], hand1.at[source], h1_recv.at[source]).wait()
        for b in range(n_prompt):
            hand2[b] = hand1[partner_ref[b]]

    def stage_two_send():
        own2.start()
        for k in range(1, n_ctx):
            h2_copy(lax.rem(me + k, n_ctx)).start()

    def earlier(step, carry):
        @pl.when(step <= me)
        def _():
            def one(g, carry):
                kv_copy(me, me - step, g).wait_recv()
                attend(me - step, g, False)
                return carry

            lax.fori_loop(0, groups, one, 0)

        @pl.when(step == 1)
        def _():
            stage_two()
            stage_two_send()

        return carry

    lax.fori_loop(1, n_ctx, earlier, 0)

    query_live = row_pos + me * tok < length
    for h in range(heads):
        result = acc[h, :, :width] / acc[h, :, width:]
        tmp[pl.ds(h, tok, stride=heads), :] = jnp.where(query_live, result, 0.0)
    att_ref[...] = tmp[...].astype(bf16).reshape(tok, heads, width)

    def drain_group(g, carry):
        def drain_one(k, carry):
            kv_copy(n_ctx - k, me, g).wait_send()
            return carry

        lax.fori_loop(1, n_ctx - me, drain_one, 0)
        return carry

    lax.fori_loop(0, groups, drain_group, 0)
    own2.wait()
    for k in range(1, n_ctx):
        h2_copy(lax.rem(me + k, n_ctx)).wait_send()
    for k in range(1, n_ctx):
        source = lax.rem(me + k, n_ctx)
        landed = dec_ref.at[:, :, 0, source]
        pltpu.make_async_copy(landed, landed, h2_recv.at[source]).wait()


def per_device(n_prompt, n_ctx, queries, keys, values, spans, partner):
    tok, heads, width = queries.shape
    groups = keys.shape[1]
    stripes = n_prompt // groups
    rows = tok // stripes
    per_ctx = partner.shape[0] // n_ctx
    vmem = pl.BlockSpec(memory_space=pltpu.VMEM)
    smem = pl.BlockSpec(memory_space=pltpu.SMEM)
    base = (lax.axis_index("ctx") * tok).astype(jnp.int32).reshape(1)
    kv = pl.pallas_call(
        prep_kernel,
        out_shape=jax.ShapeDtypeStruct((groups, 2, stripes, rows, width), bf16),
        in_specs=[smem, smem, vmem, vmem],
        out_specs=vmem,
        scratch_shapes=[pltpu.VMEM((2, tok * groups, width), f32)],
        name="prep",
    )(spans, base, keys.reshape(tok * groups, width), values.reshape(tok * groups, width))
    dma = pltpu.SemaphoreType.DMA
    attended, cache = pl.pallas_call(
        functools.partial(main_kernel, n_prompt, n_ctx),
        out_shape=(
            jax.ShapeDtypeStruct((tok, heads, width), bf16),
            jax.ShapeDtypeStruct((per_ctx, 2, 1, n_ctx, rows, width), bf16),
        ),
        in_specs=[smem, smem, vmem, pl.BlockSpec(memory_space=pl.ANY)],
        out_specs=(vmem, vmem),
        scratch_shapes=[
            pltpu.VMEM((n_ctx, groups, 2, stripes, rows, width), bf16),
            pltpu.VMEM((n_prompt, 2, rows, width), bf16),
            pltpu.VMEM((n_prompt, 2, rows, width), bf16),
            pltpu.VMEM((tok * heads, width), f32),
            pltpu.VMEM((heads, tok, width), bf16),
            pltpu.VMEM((heads, tok, 2 * width), f32),
            pltpu.VMEM((heads, tok, 1), f32),
            pltpu.VMEM((tok, tok), f32),
            dma,
            dma((n_ctx, groups)),
            dma((n_ctx, groups)),
            dma((n_prompt,)),
            dma((n_prompt,)),
            dma((n_ctx,)),
            dma((n_ctx,)),
        ],
        compiler_params=pltpu.CompilerParams(
            collective_id=0, has_side_effects=True, vmem_limit_bytes=60 * 1024 * 1024
        ),
        name="attend",
    )(spans, partner, queries, kv)
    return (attended, cache)


def solution(mesh):
    placed = (
        P(("prompt", "ctx"), None, None),
        P(("prompt", "ctx"), None, None),
        P(("prompt", "ctx"), None, None),
        P("prompt", None),
        P(),
    )
    return jax.shard_map(
        functools.partial(per_device, mesh.shape["prompt"], mesh.shape["ctx"]),
        mesh=mesh,
        in_specs=placed,
        out_specs=(P(("prompt", "ctx"), None, None), P("ctx", None, "prompt", None, None, None)),
        check_vma=False,
    )
```

```python
import functools
import math

import jax
import jax.numpy as jnp
from jax import lax
from jax.experimental import pallas as pl
from jax.experimental.pallas import tpu as pltpu
from jax.sharding import PartitionSpec as P

far_below = -1e30
MESH = pl.DeviceIdType.MESH
f32, bf16 = jnp.float32, jnp.bfloat16


def prep_kernel(spans_ref, base_ref, k_ref, v_ref, out_ref, tmp):
    groups, _, stripes, rows, _ = out_ref.shape
    length = spans_ref[0, 0] + spans_ref[0, 1]
    row = lax.broadcasted_iota(jnp.int32, (rows, 1), 0)
    for t, ref in enumerate((k_ref, v_ref)):
        tmp[t] = ref[...].astype(f32)
        for st in range(stripes):
            live = base_ref[0] + row * stripes + st < length
            for g in range(groups):
                x = tmp[t, pl.ds(st * groups + g, rows, stride=stripes * groups), :]
                out_ref[g, t, st] = jnp.where(live, x, 0.0).astype(bf16)


def main_kernel(
    n_prompt,
    n_ctx,
    spans_ref,
    partner_ref,
    q_ref,
    kv_ref,
    att_ref,
    dec_ref,
    kvbuf,
    hand1,
    hand2,
    tmp,
    qh,
    acc,
    peak,
    bias,
    own_sem,
    kv_send,
    kv_recv,
    h1_send,
    h1_recv,
    h2_send,
    h2_recv,
    relay_send,
):
    tok, heads, width = q_ref.shape
    groups, _, stripes, rows, _ = kv_ref.shape
    members = heads // groups
    per_ctx = dec_ref.shape[0]
    me_p = lax.axis_index("prompt")
    me = lax.axis_index("ctx")
    length = spans_ref[0, 0] + spans_ref[0, 1]
    scale = math.log2(math.e) / math.sqrt(width)

    own = pltpu.make_async_copy(kv_ref, kvbuf.at[me], own_sem)
    own.start()

    barrier = pltpu.get_barrier_semaphore()
    for k in range(1, n_prompt):
        pl.semaphore_signal(
            barrier, inc=1, device_id={"prompt": lax.rem(me_p + k, n_prompt)}, device_id_type=MESH
        )
    for k in range(1, n_ctx):
        pl.semaphore_signal(
            barrier, inc=1, device_id={"ctx": lax.rem(me + k, n_ctx)}, device_id_type=MESH
        )
    own.wait()
    pl.semaphore_wait(barrier, n_prompt + n_ctx - 2)

    def kv_copy(dest, block, g):
        return pltpu.make_async_remote_copy(
            src_ref=kvbuf.at[block, g],
            dst_ref=kvbuf.at[block, g],
            send_sem=kv_send.at[dest, g],
            recv_sem=kv_recv.at[block, g],
            device_id={"ctx": dest},
            device_id_type=MESH,
        )

    def h1_copy(slot):
        return pltpu.make_async_remote_copy(
            src_ref=kvbuf.at[me, lax.rem(slot, groups), :, lax.div(slot, groups)],
            dst_ref=hand1.at[me_p],
            send_sem=h1_send.at[slot],
            recv_sem=h1_recv.at[me_p],
            device_id={"prompt": slot},
            device_id_type=MESH,
        )

    def h2_copy(dest):
        return pltpu.make_async_remote_copy(
            src_ref=hand2.at[pl.ds(dest * per_ctx, per_ctx)],
            dst_ref=dec_ref.at[:, :, 0, me],
            send_sem=h2_send.at[dest],
            recv_sem=h2_recv.at[me],
            device_id={"ctx": dest},
            device_id_type=MESH,
        )

    own1 = pltpu.make_async_copy(
        kvbuf.at[me, lax.rem(me_p, groups), :, lax.div(me_p, groups)],
        hand1.at[me_p],
        h1_send.at[me_p],
    )
    own2 = pltpu.make_async_copy(
        hand2.at[pl.ds(me * per_ctx, per_ctx)], dec_ref.at[:, :, 0, me], h2_send.at[me]
    )

    square = n_ctx == 4
    half = groups // 2

    def relay_copy(dest, block, g):
        return pltpu.make_async_remote_copy(
            src_ref=kvbuf.at[block, g],
            dst_ref=kvbuf.at[block, g],
            send_sem=relay_send.at[g],
            recv_sem=kv_recv.at[block, g],
            device_id={"ctx": dest},
            device_id_type=MESH,
        )

    def each_send(act):
        def one_group(g, carry):
            for dest in range(n_ctx - 1, 0, -1):
                wanted = me < dest
                if square and dest == 3:
                    wanted = (me == 1) | (me == 2)
                if square and dest == 2:
                    wanted = me == 0

                @pl.when(wanted)
                def _():
                    act(kv_copy(dest, me, g))

            return carry

        lax.fori_loop(0, groups, one_group, 0)

    each_send(lambda copy: copy.start())
    own1.start()
    for k in range(1, n_prompt):
        h1_copy(lax.rem(me_p + k, n_prompt)).start()

    tmp[...] = q_ref[...].reshape(tok * heads, width).astype(f32)
    for h in range(heads):
        qh[h] = tmp[pl.ds(h, tok, stride=heads), :].astype(bf16)
    col = lax.broadcasted_iota(jnp.int32, (1, tok), 1)
    key_pos = lax.rem(col, rows) * stripes + lax.div(col, rows)
    row_pos = lax.broadcasted_iota(jnp.int32, (tok, 1), 0)
    bias[...] = jnp.where(
        (key_pos <= row_pos) & (key_pos + me * tok < length), 0.0, far_below
    )
    ones = jnp.ones((tok, width), bf16)
    tile = tok // 2

    def attend(block, g, first):
        keys = kvbuf[block, g, 0].reshape(tok, width)
        mixed = jnp.concatenate([kvbuf[block, g, 1].reshape(tok, width), ones], axis=1)
        if not first:
            row_bias = jnp.where(key_pos + block * tok < length, 0.0, far_below)

        def one_head(m):
            h = g * members + m
            for start in range(0, tok, tile):
                part = pl.ds(start, tile)
                scores = lax.dot_general(
                    qh[h, part, :], keys, (((1,), (1,)), ((), ())), preferred_element_type=f32
                )
                scores = scores * scale + (bias[part, :] if first else row_bias)
                top = jnp.max(scores, axis=1, keepdims=True)
                if not first:
                    before = peak[h, part, :]
                    top = jnp.maximum(top, before)
                weights = jnp.exp2(scores - top).astype(bf16)
                mixture = jnp.dot(weights, mixed, preferred_element_type=f32)
                if not first:
                    mixture = mixture + acc[h, part, :] * jnp.exp2(before - top)
                acc[h, part, :] = mixture
                peak[h, part, :] = top

        for m in range(members):
            one_head(m)

    def diagonal(g, carry):
        attend(me, g, True)
        return carry

    lax.fori_loop(0, groups, diagonal, 0)

    def stage_two():
        own1.wait()
        for k in range(1, n_prompt):
            h1_copy(lax.rem(me_p + k, n_prompt)).wait_send()
        for k in range(1, n_prompt):
            source = lax.rem(me_p + k, n_prompt)
            pltpu.make_async_copy(hand1.at[source], hand1.at[source], h1_recv.at[source]).wait()
        for b in range(n_prompt):
            hand2[b] = hand1[partner_ref[b]]

    def stage_two_send():
        own2.start()
        for k in range(1, n_ctx):
            h2_copy(lax.rem(me + k, n_ctx)).start()

    def earlier(step, carry):
        @pl.when(step <= me)
        def _():
            block = me - step
            if square:
                block = jnp.where(me == 2, step - 1, block)

            def one(g, carry):
                if square:
                    @pl.when(jnp.logical_not((me == 3) & (step == 2)))
                    def _():
                        kv_copy(me, block, g).wait_recv()

                    @pl.when((me == 1) & (g < half))
                    def _():
                        relay_copy(3, 0, g).start()

                    @pl.when((me == 2) & (step == 1) & (g >= half))
                    def _():
                        relay_copy(3, 0, g).start()
                else:
                    kv_copy(me, block, g).wait_recv()
                attend(block, g, False)
                if square:
                    @pl.when((me == 3) & (step == 1))
                    def _():
                        kv_copy(me, 1, g).wait_recv()
                        relay_copy(2, 1, g).start()

                return carry

            lax.fori_loop(0, groups, one, 0)

        @pl.when(step == 1)
        def _():
            stage_two()
            stage_two_send()

        return carry

    lax.fori_loop(1, n_ctx, earlier, 0)

    def each_relay(act):
        for g in range(groups):
            @pl.when((me == 1) if g < half else (me == 2))
            def _():
                act(relay_copy(3, 0, g))

            @pl.when(me == 3)
            def _():
                act(relay_copy(2, 1, g))

    query_live = row_pos + me * tok < length
    for h in range(heads):
        result = acc[h, :, :width] / acc[h, :, width:]
        tmp[pl.ds(h, tok, stride=heads), :] = jnp.where(query_live, result, 0.0)
    att_ref[...] = tmp[...].astype(bf16).reshape(tok, heads, width)

    each_send(lambda copy: copy.wait_send())
    if square:
        each_relay(lambda copy: copy.wait_send())
    own2.wait()
    for k in range(1, n_ctx):
        h2_copy(lax.rem(me + k, n_ctx)).wait_send()
    for k in range(1, n_ctx):
        source = lax.rem(me + k, n_ctx)
        landed = dec_ref.at[:, :, 0, source]
        pltpu.make_async_copy(landed, landed, h2_recv.at[source]).wait()


def per_device(n_prompt, n_ctx, queries, keys, values, spans, partner):
    tok, heads, width = queries.shape
    groups = keys.shape[1]
    stripes = n_prompt // groups
    rows = tok // stripes
    per_ctx = partner.shape[0] // n_ctx
    vmem = pl.BlockSpec(memory_space=pltpu.VMEM)
    smem = pl.BlockSpec(memory_space=pltpu.SMEM)
    base = (lax.axis_index("ctx") * tok).astype(jnp.int32).reshape(1)
    kv = pl.pallas_call(
        prep_kernel,
        out_shape=jax.ShapeDtypeStruct((groups, 2, stripes, rows, width), bf16),
        in_specs=[smem, smem, vmem, vmem],
        out_specs=vmem,
        scratch_shapes=[pltpu.VMEM((2, tok * groups, width), f32)],
        name="prep",
    )(spans, base, keys.reshape(tok * groups, width), values.reshape(tok * groups, width))
    dma = pltpu.SemaphoreType.DMA
    attended, cache = pl.pallas_call(
        functools.partial(main_kernel, n_prompt, n_ctx),
        out_shape=(
            jax.ShapeDtypeStruct((tok, heads, width), bf16),
            jax.ShapeDtypeStruct((per_ctx, 2, 1, n_ctx, rows, width), bf16),
        ),
        in_specs=[smem, smem, vmem, pl.BlockSpec(memory_space=pl.ANY)],
        out_specs=(vmem, vmem),
        scratch_shapes=[
            pltpu.VMEM((n_ctx, groups, 2, stripes, rows, width), bf16),
            pltpu.VMEM((n_prompt, 2, rows, width), bf16),
            pltpu.VMEM((n_prompt, 2, rows, width), bf16),
            pltpu.VMEM((tok * heads, width), f32),
            pltpu.VMEM((heads, tok, width), bf16),
            pltpu.VMEM((heads, tok, 2 * width), f32),
            pltpu.VMEM((heads, tok, 1), f32),
            pltpu.VMEM((tok, tok), f32),
            dma,
            dma((n_ctx, groups)),
            dma((n_ctx, groups)),
            dma((n_prompt,)),
            dma((n_prompt,)),
            dma((n_ctx,)),
            dma((n_ctx,)),
            dma((groups,)),
        ],
        compiler_params=pltpu.CompilerParams(
            collective_id=0, has_side_effects=True, vmem_limit_bytes=60 * 1024 * 1024
        ),
        name="attend",
    )(spans, partner, queries, kv)
    return (attended, cache)


def solution(mesh):
    placed = (
        P(("prompt", "ctx"), None, None),
        P(("prompt", "ctx"), None, None),
        P(("prompt", "ctx"), None, None),
        P("prompt", None),
        P(),
    )
    return jax.shard_map(
        functools.partial(per_device, mesh.shape["prompt"], mesh.shape["ctx"]),
        mesh=mesh,
        in_specs=placed,
        out_specs=(P(("prompt", "ctx"), None, None), P("ctx", None, "prompt", None, None, None)),
        check_vma=False,
    )
```
